32 devices in a mesh: row: 4 (over y, x), col: 2 (over core), layer: 4 (over z).
Axes of the slice: x: 2, y: 2, z: 4, core: 2. Of those that a mesh axis runs over, the one named last changes fastest.
Arguments:
- design: float32 [1024, 8192], P(('row', 'layer'), 'col'), may hold values from -6 to 6
- responses: float32 [1024, 8192], P(('row', 'layer'), 'col'), may hold values from -0.1875 to 0.1875
Outputs:
- normal_update: float32 [8192, 8192], P('row', ('col', 'layer'))
The draws below stay inside these ranges and needn't reach their ends.
All inputs are finite; a program needn't handle non-finite values.
Results may differ from the reference program's by a relative error of at most 0.00008.
Values sent between devices are 32-bit elements; how exact they have to be, the bound alone decides.
No kernel may reach another device: no remote copies, remote signals or barrier semaphores. Data moves between devices by JAX's collectives and lax.ppermute only.
A program may use at most 128 MiB of HBM per device.

```python
import jax
import jax.numpy as jnp
from jax import lax

NA = 8192
NB = 8192
K = 1024


def block_levels(rng, dims, pieces, least, high):
    gain, own = 1.0, jax.random.fold_in(rng, 6)
    for axis_at, shards_of in pieces:
        heights = jnp.exp(jax.random.uniform(jax.random.fold_in(own, axis_at), (shards_of,), jnp.float32, least / len(pieces), high / len(pieces)))
        gain = gain * jnp.repeat(heights, dims[axis_at] // shards_of).reshape([-1 if axis == axis_at else 1 for axis in range(len(dims))])
    return gain


def noise(stream_key, extent, spread, bound, split=(), dtype=jnp.bfloat16):
    values = spread * jax.random.normal(stream_key, extent, jnp.float32)
    if split:
        values = values * block_levels(stream_key, extent, split, -0.22, 0.18)
    return jnp.clip(values, -bound, bound).astype(dtype)


def setup_inputs(seed: int = 0) -> dict:
    seeds = jax.random.split(jax.random.key(seed), 3)
    return {
        "design": noise(seeds[0], (K, NA), 1.0, 6.0, ((0, 16), (1, 2)), jnp.float32),
        "responses": noise(seeds[1], (K, NB), K ** -0.5, 0.1875, ((0, 16), (1, 2)), jnp.float32),
    }


def reference(design, responses):
    transposed = jnp.transpose(design)
    return jnp.dot(transposed, responses, precision=lax.Precision.HIGHEST, preferred_element_type=jnp.float32)
```

```python
import functools

import jax
import jax.numpy as jnp
from jax import lax
from jax.experimental import pallas as pl
from jax.experimental.pallas import tpu as pltpu
from jax.sharding import PartitionSpec as P


FINAL = 512
HIGHEST = lax.Precision.HIGHEST
T0 = (((0,), (0,)), ((), ()))


def split(x):
    hi = x.astype(jnp.bfloat16)
    return hi, (x - hi.astype(jnp.float32)).astype(jnp.bfloat16)


def update_kernel(counts, spans, tiles, sides, has_acc, final, flags_ref, *refs):
    refs = list(refs)
    groups = [[refs.pop(0) for _ in range(count)] for count in counts]
    resp = [refs.pop(0) for _ in spans]
    acc_ref = refs.pop(0) if has_acc else None
    out_ref, held = refs[-2:]
    step = pl.program_id(0)
    depth = held.shape[0] // 3
    size = groups[0][0].shape[1] // tiles

    @pl.when(step == 0)
    def _():
        hi, lo = split(jnp.concatenate([p[start : start + rows, :] for p, (start, rows) in zip(resp, spans)], axis=0))
        held[:depth, :] = hi
        held[depth : 2 * depth, :] = lo
        held[2 * depth :, :] = hi

    def tile(pieces, at):
        at = pl.ds(pl.multiple_of(at * size, size), size)
        blocks = [p[:, at] for p in pieces]
        if final:
            blocks = [jnp.where(flags_ref[1] == 1, *blocks)]
        hi, lo = split(jnp.concatenate(blocks, axis=0))
        total = lax.dot_general(jnp.concatenate([hi, hi, lo], axis=0), held[...], T0, preferred_element_type=jnp.float32)
        if has_acc:
            total += acc_ref[pl.ds(pl.multiple_of((sides[0] * tiles + step) * size, size), size), :]
        if final:
            out_ref[...] = total
        else:
            out_ref[pl.ds(pl.multiple_of(step * size, size), size), :] = total

    for i, pieces in enumerate(groups):
        pl.when((step >= i * tiles) & (step < (i + 1) * tiles))(lambda i=i, pieces=pieces: tile(pieces, step - i * tiles))


def update(flags, groups, resp, acc, size, sides=(0, 1), final=False, base=None):
    half, width = groups[0][0].shape[1], resp[0][0].shape[1]
    arrays, spans = [r[0] for r in resp], [r[1:] for r in resp]
    depth = sum(rows for _, rows in spans)
    tiles = half // size
    has_acc, has_base = acc is not None, base is not None
    whole = pl.BlockSpec(memory_space=pltpu.VMEM)
    flip = sides[0]
    placed = pl.BlockSpec((size, width), lambda i, flags: ((flip + flags[0] - 2 * flip * flags[0]) * tiles + i, 0))
    shape = (2 * half, width)
    operands = [x for group in groups for x in group] + arrays + ([acc] if has_acc else [])
    return pl.pallas_call(
        functools.partial(update_kernel, [len(g) for g in groups], spans, tiles, sides, has_acc, final),
        out_shape=jax.ShapeDtypeStruct(shape, jnp.float32) if final else pltpu.VMEM(shape, jnp.float32),
        grid_spec=pltpu.PrefetchScalarGridSpec(
            num_scalar_prefetch=1,
            grid=(len(sides) * tiles,),
            in_specs=[whole] * len(operands) + [pl.BlockSpec(memory_space=pl.ANY)] * has_base,
            out_specs=placed if final else whole,
            scratch_shapes=[pltpu.VMEM((3 * depth, width), jnp.bfloat16)],
        ),
        input_output_aliases={1 + len(operands): 0} if has_base else {len(operands): 0} if has_acc and not final else {},
        compiler_params=pltpu.CompilerParams(vmem_limit_bytes=12 << 20),
        cost_estimate=pl.CostEstimate(
            flops=6 * depth * len(sides) * half * width,
            bytes_accessed=4 * (depth * (2 * half + width) + (1 + has_acc) * len(sides) * half * width),
            transcendentals=0,
        ),
    )(flags, *operands, *([base] if has_base else []))


def by_permutes(sizes, design, responses):
    layers = sizes["layer"]
    last = layers - 1
    row, core, layer = lax.axis_index("row"), lax.axis_index("col"), lax.axis_index("layer")
    rows, half = design.shape[0], design.shape[1] // 4
    width = responses.shape[1] // layers

    swap = lambda x: lax.ppermute(x, "col", [(0, 1), (1, 0)])
    over_row = lambda x, m: lax.ppermute(x, "row", [(i, i ^ m) for i in range(sizes["row"])])
    along = lambda x, pairs: lax.ppermute(x, "layer", pairs)

    columns = lambda d: lax.dynamic_slice(responses, (0, ((layer - d) % layers) * width), (rows, width))
    z = [columns(0)] + [along(columns(d), [((i + d) % layers, i) for i in range(layers)]) for d in (1, 2, 3)]
    r0 = [z[0]] + [over_row(z[0], m) for m in (1, 2, 3)]
    far = jnp.concatenate([jnp.where(layer == last, z[3], z[1]), z[2], jnp.where(layer == last, z[1], z[3])], axis=0)
    r = [far] + [over_row(far, m) for m in (1, 2, 3)]

    piece = lambda at, h: lax.dynamic_slice(design, (0, (2 * at + h) * half), (rows, half))
    got = [swap(piece(at, 1 - core)) for at in (0, 1)]
    mine = []
    for m in range(4):
        to = row ^ m
        sent = jnp.where(to // 2 == core, piece(to % 2, core), jnp.where(to % 2 == 0, got[0], got[1]))
        mine.append(over_row(sent, m) if m else sent)
    outer = (layer == 0) | (layer == last)
    a = {0: [jnp.concatenate(mine[:2], axis=0), jnp.concatenate(mine[2:], axis=0)], 1: [], 2: [], 3: []}
    for h in (0, 1):
        left = along(a[0][h], [(1, 0), (2, 1), (3, 2)])
        right = along(a[0][h], [(0, 1), (1, 2), (2, 3)])
        a[1].append(jnp.where(layer == last, right, left))
        left2 = along(left, [(1, 0), (2, 1)])
        right2 = along(right, [(1, 2), (2, 3)])
        a[2].append(jnp.where(layer < 2, left2, right2))
        ends = along(a[2][h], [(1, 0), (2, 3)])
        if h == 0:
            ends, right = lax.optimization_barrier((ends, right))
            a[3].append(jnp.where(outer, ends, right))
    b = {slot: [swap(x) for x in a[slot]] for slot in range(4)}

    def resp(slot, halves):
        ms = [m for h in halves for m in (2 * h, 2 * h + 1)]
        return [(r[m], (slot - 1) * rows, rows) if slot else (r0[m], 0, rows) for m in ms]

    flags = jnp.stack([core, outer.astype(core.dtype)])
    total = None
    for slot, halves in ((0, (0, 1)), (1, (0, 1)), (2, (0, 1)), (3, (0,))):
        total = update(flags, [[a[slot][h] for h in halves], [b[slot][h] for h in halves]], resp(slot, halves), total, 512)
    swapped = [swap(ends), swap(right)]
    out = None
    for side, pieces in ((0, [ends, right]), (1, swapped)):
        out = update(flags, [pieces], resp(3, (1,)), total, FINAL, sides=(side,), final=True, base=out)
    return out


def by_collectives(sizes, design, responses):
    rows, layers = sizes["row"], sizes["layer"]
    widened = lax.all_gather(design, "col", axis=1, tiled=True)
    panel = lax.all_to_all(widened, "row", split_axis=1, concat_axis=0, tiled=True)
    panel = lax.all_gather(panel, "layer", axis=0, tiled=True)
    block = lax.all_to_all(responses, "layer", split_axis=1, concat_axis=0, tiled=True)
    block = lax.all_gather(block, "row", axis=0, tiled=True)
    block = block.reshape(rows, layers, -1, block.shape[1]).swapaxes(0, 1).reshape(block.shape)
    return lax.dot_general(panel, block, T0, precision=HIGHEST, preferred_element_type=jnp.float32)


def solution(mesh):
    sizes = dict(mesh.shape)
    small = (sizes["row"], sizes["col"], sizes["layer"]) == (4, 2, 4)
    plan = by_permutes if small else by_collectives

    def body(design, responses):
        return plan(sizes, design, responses)

    return jax.shard_map(
        body,
        mesh=mesh,
        in_specs=(P(("row", "layer"), "col"), P(("row", "layer"), "col")),
        out_specs=P("row", ("col", "layer")),
        check_vma=False,
    )
```
